32 devices in a mesh: rep: 2 (over y), grp: 4 (over z), tp: 2 (over x), sub: 2 (over core).
Axes of the slice: x: 2, y: 2, z: 4, core: 2. Of those that a mesh axis runs over, the one named last changes fastest.
Arguments:
- new_q: bfloat16 [4096, 8192], P(('rep', 'grp', 'sub'), 'tp'), parts along dimension 0
- new_kv: bfloat16 [2, 4096, 1024], P(None, ('rep', 'grp', 'sub'), 'tp'), parts along dimension 1
- hist_kv: bfloat16 [2, 8, 4, 4, 128, 1024], P(None, ('rep', 'grp'), None, None, 'sub', 'tp'), parts along dimension 1, may hold values from -6 to 6
- page_place: int32 [8, 16], P(('rep', 'grp')), parts along dimension 0, may hold values from 0 to 15, each once within a row
- hist_len: int32 [8], P(('rep', 'grp')), parts along dimension 0, may hold values from 1 to 2048, 4096 in all
- new_len: int32 [8], P(('rep', 'grp')), parts along dimension 0, may hold values from 128 to 512, as said below
- dec_q: bfloat16 [128, 8192], P(('rep', 'grp', 'sub'), 'tp'), parts along dimension 0
- dec_cache: bfloat16 [2, 128, 512, 1024], P(None, ('rep', 'grp', 'sub'), None, 'tp'), parts along dimension 1
- dec_len: int32 [128], P(('rep', 'grp', 'sub')), parts along dimension 0, may hold values from 64 to 512, as said below
Outputs:
- prefill_out: bfloat16 [4096, 8192], P(('rep', 'grp', 'sub'), 'tp'), parts along dimension 0
- decode_out: bfloat16 [128, 8192], P(('rep', 'grp', 'sub'), 'tp'), parts along dimension 0
The draws below stay inside these ranges and needn't reach their ends.
There are 2 independent parts, one for each index of `rep`. The reference program is written for one: setup_inputs(seed, part) draws one part's arguments, and reference() takes and returns one part's arrays. A program takes and returns all parts, laid end to end along the dimension named above; each array names one. Nothing has to cross between parts.
Inputs may be any that keep to these rules, and one draw needn't show every extreme that they name: `page_place`: each row is an ordering of the slots 0 to 15: each owner holds exactly 4 pages of every conversation. `hist_len`: some conversation has exactly 2048. `new_len`: some conversation has exactly 512. `dec_len`: some request has exactly 512.
All inputs are finite; a program needn't handle non-finite values. No bound on the sum of `hist_len` on one device may be relied on, other than what follows from the above.
Results may differ from the reference program's by a relative error of at most 0.008.
Values may be sent and summed in bfloat16 or wider, within the bound.
A program may use at most 128 MiB of HBM per device.

```python
import math
import jax
import jax.numpy as jnp
import numpy as np
from jax import lax

HQ = 64
KVH = 8
HD = 128
NEW = 512
PAGE = 128
P_MAX = 16
CACHE = 512
NG = 4
CAP = 4
HIST_MAX = 2048
DEC_REQ = 64


def fresh_keys(key):
    base = jax.random.normal(jax.random.fold_in(key, 11), (NG * NEW, KVH * HD), jnp.float32)
    return base


def cache_keys(key):
    base = jax.random.normal(jax.random.fold_in(key, 31), (DEC_REQ, CACHE, KVH * HD), jnp.float32)
    return base


def draw_values(key, shape):
    return jax.random.normal(key, shape, jnp.float32)


def draw_new_kv(key, part):
    keys = fresh_keys(key)
    values = draw_values(jax.random.fold_in(key, 13), keys.shape)
    return jnp.stack([keys, values]).astype(jnp.bfloat16)


def draw_new_q(key, part):
    base = jax.random.normal(jax.random.fold_in(key, 21), (NG * NEW, HQ, HD), jnp.float32)
    return base.reshape(NG * NEW, HQ * HD).astype(jnp.bfloat16)


def draw_dec_cache(key, part):
    keys = cache_keys(key)
    values = draw_values(jax.random.fold_in(key, 33), keys.shape)
    return jnp.stack([keys, values]).astype(jnp.bfloat16)


def draw_dec_q(key, part):
    base = jax.random.normal(jax.random.fold_in(key, 41), (DEC_REQ, HQ, HD), jnp.float32)
    return base.reshape(DEC_REQ, HQ * HD).astype(jnp.bfloat16)


def draw_new_len(key, part):
    counts = jax.random.randint(jax.random.fold_in(key, 51), (NG,), NEW // 4, NEW + 1)
    chosen = jax.random.randint(jax.random.fold_in(key, 52), (), 0, NG)
    return jnp.where(jnp.arange(NG) == chosen, NEW, counts).astype(jnp.int32)


def draw_dec_len(key, part):
    counts = jax.random.randint(jax.random.fold_in(key, 61), (DEC_REQ,), CACHE // 8, CACHE + 1)
    chosen = jax.random.randint(jax.random.fold_in(key, 62), (), 0, DEC_REQ)
    return jnp.where(jnp.arange(DEC_REQ) == chosen, CACHE, counts).astype(jnp.int32)


def shard_levels(key, shape, split, smallest, largest):
    def one(position, blocks):
        heights = jax.random.uniform(jax.random.fold_in(jax.random.fold_in(key, 6), position), (blocks,), jnp.float32, smallest / len(split), largest / len(split))
        return jnp.repeat(jnp.exp(heights), shape[position] // blocks).reshape((-1,) + (1,) * (len(shape) - position - 1))

    factor_of = one(*split[0])
    for cut in split[1:]:
        factor_of = factor_of * one(*cut)
    return factor_of


def length_profile(amount, total, most, slope):
    loads = [(1 << 20) // math.isqrt(rank ** slope) + 1 for rank in range(2, amount + 1)]
    surplus, given = total - most - (amount - 1), [1] * (amount - 1)
    while surplus > 0:
        candidates = [i for i in range(amount - 1) if given[i] < most]
        pool, remaining = sum([loads[i] for i in candidates]), surplus
        for i in candidates:
            addition = min(most - given[i], max(1, remaining * loads[i] // pool), surplus)
            given[i] = given[i] + addition
            surplus = surplus - addition
    return np.array([most] + given)


def ragged(stream_key, amount, total, bound, lean):
    if amount == 2:
        one = jax.random.randint(stream_key, (), max(1, total - bound), min(bound, total - 1) + 1)
        return jnp.stack([one, total - one])
    tallies = jnp.asarray(length_profile(amount, total, bound, lean), jnp.int32)
    pairs = (amount - 1) // 2
    donor, taker = tallies[1:1 + 2 * pairs:2], tallies[2:2 + 2 * pairs:2]
    slack = jnp.minimum(donor - 1, bound - taker)
    shifted = jax.random.randint(jax.random.fold_in(stream_key, 1), (pairs,), 0, 1 << 20) % (slack + 1)
    tallies = tallies.at[1:1 + 2 * pairs:2].set(donor - shifted).at[2:2 + 2 * pairs:2].set(taker + shifted)
    return tallies[jax.random.permutation(jax.random.fold_in(stream_key, 2), amount)]


def gaussian(stream_key, extent, scale, most, shards=(), kind=jnp.bfloat16):
    level = shard_levels(stream_key, extent, shards, -0.22, 0.18) if shards else 1.0
    drawn = jax.random.normal(stream_key, extent, jnp.float32) * scale * level
    return jnp.minimum(jnp.maximum(drawn, -most), most).astype(kind)


def setup_inputs(seed: int = 0, part: int = 0) -> dict:
    splits = jax.random.split(jax.random.key(seed), 10)
    part_splits = jax.random.split(jax.random.fold_in(splits[9], part), 10)
    new_q = draw_new_q(jax.random.fold_in(jax.random.fold_in(splits[9], part), 71), part)
    new_kv = draw_new_kv(jax.random.fold_in(jax.random.fold_in(splits[9], part), 71), part)
    hist_kv = gaussian(part_splits[2], (2, NG, NG, CAP, PAGE, KVH * HD), 1.0, 6.0, ((1, 4), (4, 2), (5, 2)))
    page_place = jax.vmap(lambda own: jax.random.permutation(own, P_MAX))(jax.random.split(part_splits[3], NG)).reshape((NG, P_MAX)).astype(jnp.int32)
    hist_len = ragged(part_splits[4], NG, NG * HIST_MAX // 2, HIST_MAX, 2).astype(jnp.int32)
    new_len = draw_new_len(jax.random.fold_in(jax.random.fold_in(splits[9], part), 71), part)
    dec_q = draw_dec_q(jax.random.fold_in(jax.random.fold_in(splits[9], part), 71), part)
    dec_cache = draw_dec_cache(jax.random.fold_in(jax.random.fold_in(splits[9], part), 71), part)
    dec_len = draw_dec_len(jax.random.fold_in(jax.random.fold_in(splits[9], part), 71), part)
    return dict(new_q=new_q, new_kv=new_kv, hist_kv=hist_kv, page_place=page_place, hist_len=hist_len, new_len=new_len, dec_q=dec_q, dec_cache=dec_cache, dec_len=dec_len)


NEG = -1e30


def weigh(scores, allowed, values_form, values):
    scores = jnp.where(allowed, scores, NEG)
    top = jnp.max(scores, axis=-1, keepdims=True)
    weights = jnp.exp(scores - top)
    total = jnp.sum(weights, axis=-1)
    rounded = lax.optimization_barrier(weights.astype(jnp.bfloat16))
    mixed = jnp.einsum(values_form, rounded.astype(jnp.float32), values.astype(jnp.float32))
    return mixed / total[..., None]


def reference(new_q, new_kv, hist_kv, page_place, hist_len, new_len, dec_q, dec_cache, dec_len):
    group = HQ // KVH
    scale = HD ** -0.5
    positions = jnp.arange(NEW, dtype=jnp.int32)
    hist_pos = jnp.arange(P_MAX * PAGE, dtype=jnp.int32)

    def one_conv(conv):
        owned = jnp.take(hist_kv, conv, axis=2).reshape(2, NG * CAP, PAGE, KVH, HD)
        place = jnp.take(page_place, conv, axis=0)
        ordered = jnp.take(owned, place, axis=1).reshape(2, P_MAX * PAGE, KVH, HD)
        fresh = lax.dynamic_slice_in_dim(new_kv, conv * NEW, NEW, 1).reshape(2, NEW, KVH, HD)
        keys = jnp.concatenate([ordered[0], fresh[0]], axis=0)
        values = jnp.concatenate([ordered[1], fresh[1]], axis=0)
        limit = jnp.take(hist_len, conv)
        count = jnp.take(new_len, conv)
        seen_hist = jnp.broadcast_to((hist_pos < limit)[None, :], (NEW, P_MAX * PAGE))
        seen_new = (positions[None, :] <= positions[:, None]) & (positions[None, :] < count)
        allowed = jnp.concatenate([seen_hist, seen_new], axis=1)
        queries = lax.dynamic_slice_in_dim(new_q, conv * NEW, NEW, 0).reshape(NEW, KVH, group, HD)
        scores = jnp.einsum('qkgd,skd->kgqs', queries.astype(jnp.float32), keys.astype(jnp.float32)) * scale
        mixed = weigh(scores, allowed[None, None], 'kgqs,skd->kgqd', values)
        out = jnp.transpose(mixed, (2, 0, 1, 3)).reshape(NEW, HQ * HD)
        out = jnp.where((positions < count)[:, None], out, 0.0)
        return out.astype(jnp.bfloat16)

    prefill_out = lax.map(one_conv, jnp.arange(NG, dtype=jnp.int32)).reshape(NG * NEW, HQ * HD)

    requests = dec_q.shape[0]
    dq = dec_q.reshape(requests, KVH, group, HD).astype(jnp.float32)
    dkeys = dec_cache[0].reshape(requests, CACHE, KVH, HD).astype(jnp.float32)
    dvalues = dec_cache[1].reshape(requests, CACHE, KVH, HD)
    dscores = jnp.einsum('rkgd,rskd->rkgs', dq, dkeys) * scale
    dallowed = (jnp.arange(CACHE, dtype=jnp.int32)[None, :] < dec_len[:, None])[:, None, None, :]
    dmixed = weigh(dscores, dallowed, 'rkgs,rskd->rkgd', dvalues)
    decode_out = dmixed.reshape(requests, HQ * HD).astype(jnp.bfloat16)
    return prefill_out, decode_out
```

```python
import functools
import math

import jax
import jax.numpy as jnp
from jax import lax
from jax.experimental import pallas as pl
from jax.experimental.pallas import tpu as pltpu
from jax.sharding import PartitionSpec as P

HQ = 64
KVH = 8
HD = 128
PAGE = 128
GROUP = HQ // KVH
NEG = -1e30
FACTOR = HD ** (-0.5) * math.log2(math.e)
MESH = pl.DeviceIdType.MESH
UNROLL = 4


def dot_nt(a, b):
    return lax.dot_general(a, b, (((1,), (1,)), ((), ())), preferred_element_type=jnp.float32)


def kernel(
    n, n_sub, place_ref, hist_len_ref, new_len_ref, dec_len_ref,
    dec_q_ref, q_hbm, new_hbm, hist_hbm, cache_hbm,
    out_ref, dec_out_ref,
    q_buf, new_buf, hist_buf, relay_buf, cache_buf, acc_buf, top_buf, new_bias, hist_bias,
    local_sem, cache_sem, send_sem, recv_sem,
):
    rows = q_buf.shape[0]
    kv_local = new_buf.shape[-1] // HD
    slots, tokens = hist_buf.shape[2], hist_buf.shape[4]
    requests, cached = cache_buf.shape[1], cache_buf.shape[2]
    grp = lax.axis_index("grp")
    sub = lax.axis_index("sub")

    order = [0]
    for d in range(1, n // 2 + 1):
        order.append(d)
        if n - d != d:
            order.append(n - d)
    last = n - 1
    relayed = n % 4 == 0

    def at(shift):
        return lax.rem(grp + shift + n, n)

    barrier = pltpu.get_barrier_semaphore()
    for d in range(1, n):
        pl.semaphore_signal(barrier, inc=1, device_id={"grp": at(d)}, device_id_type=MESH)
    for e in range(1, n_sub):
        pl.semaphore_signal(
            barrier, inc=1, device_id={"sub": lax.rem(sub + e, n_sub)}, device_id_type=MESH
        )

    copy_q = pltpu.make_async_copy(q_hbm, q_buf, local_sem.at[0])
    copy_new = pltpu.make_async_copy(new_hbm, new_buf.at[:, sub], local_sem.at[1])
    copy_own = pltpu.make_async_copy(
        hist_hbm.at[:, 0, grp], hist_buf.at[:, 0, :, sub], local_sem.at[2]
    )

    def cache_copy(r):
        return pltpu.make_async_copy(cache_hbm.at[:, r], cache_buf.at[:, r], cache_sem.at[r])

    counter = [0]

    def remote(src, dst, device):
        i = counter[0]
        counter[0] += 1
        return pltpu.make_async_remote_copy(
            src_ref=src, dst_ref=dst, send_sem=send_sem.at[i], recv_sem=recv_sem.at[i],
            device_id=device, device_id_type=MESH,
        )

    def to_subs(src, dst):
        return [
            remote(src, dst, {"sub": lax.rem(sub + e, n_sub)}) for e in range(1, n_sub)
        ]

    first_hop, second_hop, direct = [], [], []
    if relayed:
        quarter = n // 4
        for kv, step in ((0, quarter), (1, n - quarter)):
            first_hop.append(
                remote(hist_hbm.at[kv, 0, at(n // 2)], relay_buf.at[kv], {"grp": at(step)})
            )
            second_hop.append(
                remote(relay_buf.at[kv], hist_buf.at[kv, last, :, sub], {"grp": at(step)})
            )
    for i in range(1, n - 1 if relayed else n):
        direct.append(
            remote(
                hist_hbm.at[:, 0, at(order[i])], hist_buf.at[:, i, :, sub], {"grp": at(order[i])}
            )
        )
    share_new = to_subs(new_hbm, new_buf.at[:, sub])
    share_own = to_subs(hist_hbm.at[:, 0, grp], hist_buf.at[:, 0, :, sub])
    share = {
        i: to_subs(hist_buf.at[:, i, :, sub], hist_buf.at[:, i, :, sub]) for i in range(1, n)
    }

    copy_q.start()
    copy_new.start()
    copy_own.start()
    pl.semaphore_wait(barrier, n - 1 + n_sub - 1)
    for copy in first_hop + direct + share_new + share_own:
        copy.start()

    @pl.loop(0, requests)
    def _(r):
        cache_copy(r).start()

    limit = hist_len_ref[0]
    count = new_len_ref[0]
    lane = lax.broadcasted_iota(jnp.int32, (1, PAGE), 1)
    for i in range(n):
        owner = at(-order[i])
        for s in range(slots):
            slot = owner * slots + s
            page = jnp.int32(0)
            for p in range(place_ref.shape[1]):
                page = page + jnp.where(place_ref[0, p] == slot, p, 0)
            hist_bias[i, :, s * PAGE : (s + 1) * PAGE] = jnp.where(
                page * PAGE + lane < limit, 0.0, NEG
            )
    query_pos = sub * rows + lax.broadcasted_iota(jnp.int32, (rows, n_sub * rows), 0)
    key_pos = lax.broadcasted_iota(jnp.int32, (rows, n_sub * rows), 1)
    new_bias[...] = jnp.where((key_pos <= query_pos) & (key_pos < count), 0.0, NEG)

    head_row = lax.broadcasted_iota(jnp.int32, (kv_local * GROUP, HD), 0) // GROUP
    cached_pos = lax.broadcasted_iota(jnp.int32, (1, cached), 1)

    def decode(begin, end):
        @pl.loop(begin, end)
        def _(r):
            cache_copy(r).wait()
            q = dec_q_ref[r]
            zero = jnp.zeros_like(q)
            wide = jnp.concatenate(
                [jnp.where(head_row == k, q, zero) for k in range(kv_local)], axis=1
            )
            s = dot_nt(wide, cache_buf[0, r]) * FACTOR
            s = s + jnp.where(cached_pos < dec_len_ref[r], 0.0, NEG)
            top = jnp.max(s, axis=-1, keepdims=True)
            w = jnp.exp2(s - top)
            total = jnp.sum(w, axis=-1, keepdims=True)
            mixed = jnp.dot(
                w.astype(jnp.bfloat16), cache_buf[1, r], preferred_element_type=jnp.float32
            )
            picked = jnp.zeros((kv_local * GROUP, HD), jnp.float32)
            for k in range(kv_local):
                picked = jnp.where(head_row == k, mixed[:, k * HD : (k + 1) * HD], picked)
            dec_out_ref[r] = (picked / total).astype(jnp.bfloat16)

    def new_chunk(kv, columns):
        return new_buf[kv, :, :, columns].reshape(n_sub * rows, HD)

    def hist_chunk(kv, begin, end, columns):
        block = hist_buf[kv, begin:end, :, :, :, columns]
        return block.reshape((end - begin) * slots * n_sub * tokens, HD)

    def bias_row(begin, end):
        return jnp.concatenate([hist_bias[i] for i in range(begin, end)], axis=1)

    inner = GROUP // UNROLL
    row_pos = sub * rows + lax.broadcasted_iota(jnp.int32, (rows, HD), 0)

    def sweep(k_begin, k_end, with_new, begin, end, first, final):
        @pl.loop(k_begin * inner, k_end * inner)
        def _(step):
            k = step // inner
            columns = pl.ds(pl.multiple_of(k * HD, HD), HD)
            for u in range(UNROLL):
                h = step * UNROLL + u
                head = pl.ds(pl.multiple_of(h * HD, HD), HD)
                q = q_buf[:, head]
                parts = []
                if with_new:
                    parts.append((dot_nt(q, new_chunk(0, columns)) * FACTOR + new_bias[...],
                                  new_chunk(1, columns)))
                parts.append((dot_nt(q, hist_chunk(0, begin, end, columns)) * FACTOR
                              + bias_row(begin, end), hist_chunk(1, begin, end, columns)))
                top = None
                for s, _v in parts:
                    here = jnp.max(s, axis=-1, keepdims=True)
                    top = here if top is None else jnp.maximum(top, here)
                if not first:
                    old = top_buf[h]
                    top = jnp.maximum(old, top)
                    shrink = jnp.exp2(old - top)
                    acc = acc_buf[h] * jnp.concatenate([shrink, shrink], axis=1)
                    top_col = top[:, :1]
                else:
                    top_col = top
                    top = jnp.broadcast_to(top, (rows, HD))
                    acc = None
                for s, v in parts:
                    w = jnp.exp2(s - top_col).astype(jnp.bfloat16)
                    wide = jnp.concatenate([v, jnp.ones_like(v)], axis=1)
                    term = jnp.dot(w, wide, preferred_element_type=jnp.float32)
                    acc = term if acc is None else acc + term
                if final:
                    mixed = acc[:, :HD] / acc[:, HD:]
                    out_ref[:, head] = jnp.where(row_pos < count, mixed, 0.0).astype(jnp.bfloat16)
                else:
                    acc_buf[h] = acc
                    top_buf[h] = top

    half = (kv_local + 1) // 2
    cut = requests // 2
    decode(0, cut)
    copy_q.wait()
    copy_new.wait()
    copy_own.wait()
    for copy in share_new + share_own:
        copy.wait_recv()
    sweep(0, half, True, 0, 1, True, False)
    for before, after in zip(first_hop, second_hop):
        before.wait_recv()
        after.start()
    sweep(half, kv_local, True, 0, 1, True, False)
    for i in range(1, n - 1):
        direct[i - 1].wait_recv()
        for copy in share[i]:
            copy.start()
    decode(cut, requests)
    for i in range(1, n - 1):
        for copy in share[i]:
            copy.wait_recv()
    sweep(0, half, False, 1, n - 1, False, False)
    for copy in second_hop if relayed else direct[n - 2 :]:
        copy.wait_recv()
    for copy in share[last]:
        copy.start()
    sweep(half, kv_local, False, 1, n - 1, False, False)
    for copy in share[last]:
        copy.wait_recv()
    sweep(0, kv_local, False, last, n, False, True)
    for copy in first_hop + second_hop + direct + share_new + share_own:
        copy.wait_send()
    for i in range(1, n):
        for copy in share[i]:
            copy.wait_send()


def shards(n, n_sub, new_q, new_kv, hist_kv, page_place, hist_len, new_len, dec_q, dec_cache, dec_len):
    rows = new_q.shape[0]
    width = new_kv.shape[2]
    heads = new_q.shape[1] // HD
    requests, cached = dec_cache.shape[1], dec_cache.shape[2]
    slots, tokens = hist_kv.shape[3], hist_kv.shape[4]
    copies = 4 + n + (n + 1) * (n_sub - 1)
    smem = pl.BlockSpec(memory_space=pltpu.SMEM)
    vmem = pl.BlockSpec(memory_space=pltpu.VMEM)
    anywhere = pl.BlockSpec(memory_space=pl.ANY)
    out, dec_out = pl.pallas_call(
        functools.partial(kernel, n, n_sub),
        out_shape=(
            jax.ShapeDtypeStruct((rows, heads * HD), jnp.bfloat16),
            jax.ShapeDtypeStruct((requests, heads, HD), jnp.bfloat16),
        ),
        in_specs=[smem] * 4 + [vmem] + [anywhere] * 4,
        out_specs=(vmem, vmem),
        scratch_shapes=[
            pltpu.VMEM((rows, heads * HD), jnp.bfloat16),
            pltpu.VMEM((2, n_sub, rows, width), jnp.bfloat16),
            pltpu.VMEM((2, n, slots, n_sub, tokens, width), jnp.bfloat16),
            pltpu.VMEM((2, slots, tokens, width), jnp.bfloat16),
            pltpu.VMEM((2, requests, cached, width), jnp.bfloat16),
            pltpu.VMEM((heads, rows, 2 * HD), jnp.float32),
            pltpu.VMEM((heads, rows, HD), jnp.float32),
            pltpu.VMEM((rows, n_sub * rows), jnp.float32),
            pltpu.VMEM((n, 1, slots * PAGE), jnp.float32),
            pltpu.SemaphoreType.DMA((3,)),
            pltpu.SemaphoreType.DMA((requests,)),
            pltpu.SemaphoreType.DMA((copies,)),
            pltpu.SemaphoreType.DMA((copies,)),
        ],
        compiler_params=pltpu.CompilerParams(
            collective_id=0, has_side_effects=True, vmem_limit_bytes=60 << 20
        ),
    )(page_place, hist_len, new_len, dec_len, dec_q.reshape(requests, heads, HD),
      new_q, new_kv, hist_kv, dec_cache)
    return out, dec_out.reshape(requests, heads * HD)


def solution(mesh):
    in_specs = (
        P(("rep", "grp", "sub"), "tp"),
        P(None, ("rep", "grp", "sub"), "tp"),
        P(None, ("rep", "grp"), None, None, "sub", "tp"),
        P(("rep", "grp"), None),
        P(("rep", "grp")),
        P(("rep", "grp")),
        P(("rep", "grp", "sub"), "tp"),
        P(None, ("rep", "grp", "sub"), None, "tp"),
        P(("rep", "grp", "sub")),
    )
    out_specs = (P(("rep", "grp", "sub"), "tp"), P(("rep", "grp", "sub"), "tp"))
    body = functools.partial(shards, mesh.shape["grp"], mesh.shape["sub"])
    return jax.shard_map(body, mesh=mesh, in_specs=in_specs, out_specs=out_specs, check_vma=False)
```
